32 devices in a mesh: task: 4 (over y, core), col: 8 (over z, x).
Axes of the slice: x: 2, y: 2, z: 4, core: 2. Of those that a mesh axis runs over, the one named last changes fastest.
Arguments:
- layer_inputs: bfloat16 [4, 1024, 8192], P('task', None, 'col'), may hold values from -6 to 6
- queries: bfloat16 [4, 1024, 8192], P('task', None, 'col'), may hold values from -1000 to 1000, as said below
- key_values: bfloat16 [4, 1024, 2048], P('task', 'col'), may hold values from -8 to 8, as said below
- out_grads: bfloat16 [4, 1024, 8192], P('task', None, 'col'), may hold values from -0.29882812 to 0.29882812
- lengths: int32 [4, 4], P('task'), may hold values from 1 to 512, 1024 in all within a row
- task_weights: bfloat16 [4, 8192, 2048], P('task', 'col'), may hold values from -6 to 6
Outputs:
- fisher: float32 [4, 8192, 2048], P('task', 'col')
- merged: bfloat16 [8192, 2048], P('col')
The draws below stay inside these ranges and needn't reach their ends.
Inputs may be any that keep to these rules, and one draw needn't show every extreme that they name: `queries`: queries of every head for the tokens of each task. `key_values`: keys and values of every head for the tokens of each task.
All inputs are finite; a program needn't handle non-finite values.
Results may differ from the reference program's by a relative error of at most 0.02.
Values may be sent and summed in bfloat16 or wider, within the bound.
No kernel may reach another device: no remote copies, remote signals or barrier semaphores. Data moves between devices by JAX's collectives and lax.ppermute only.
A program may use at most 128 MiB of HBM per device.

```python
import math
import jax
import jax.numpy as jnp
import numpy as np
from jax import lax

D = 8192
QH = 64
KVH = 8
HD = 128
TOK = 1024
NSEQ = 4
MAXLEN = 512
KVC = 2048
TASKS = 4
N_COL = 8


def shared_fields(key):
    base = jax.random.fold_in(key, 7)
    first, second = jax.random.split(base, 2)
    key_values = jax.random.normal(first, (TASKS, TOK, KVH, 2, HD), jnp.float32)
    key_values = jnp.clip(key_values, -6.0, 6.0)
    queries = jax.random.normal(second, (TASKS, TOK, KVH, QH // KVH, HD), jnp.float32)
    queries = jnp.clip(queries, -6.0, 6.0)
    return (queries.reshape(TASKS, TOK, QH * HD), key_values.reshape(TASKS, TOK, KVH * 2 * HD))


def draw_queries(key, part):
    return shared_fields(key)[0].astype(jnp.bfloat16)


def draw_key_values(key, part):
    return shared_fields(key)[1].astype(jnp.bfloat16)


def levels(key, shape, shards, low, largest):
    def one(axis_at, blocks):
        draws = jax.random.uniform(jax.random.fold_in(jax.random.fold_in(key, 6), axis_at), (blocks,), jnp.float32, low / len(shards), largest / len(shards))
        return jnp.repeat(jnp.exp(draws), shape[axis_at] // blocks).reshape((-1,) + (1,) * (len(shape) - axis_at - 1))

    level = one(*shards[0])
    for cut in shards[1:]:
        level = level * one(*cut)
    return level


def length_profile(amount, total, most, lean):
    portions = [(1 << 20) // math.isqrt(grade ** lean) + 1 for grade in range(2, amount + 1)]
    surplus, holding = total - most - (amount - 1), [1] * (amount - 1)
    while surplus > 0:
        movable = [i for i in range(amount - 1) if holding[i] < most]
        whole, left = sum([portions[i] for i in movable]), surplus
        for i in movable:
            more = min(most - holding[i], max(1, left * portions[i] // whole), surplus)
            holding[i] = holding[i] + more
            surplus = surplus - more
    return np.array([most] + holding)


def uneven(key, amount, total, reach, skew):
    if amount == 2:
        one = jax.random.randint(key, (), max(1, total - reach), min(reach, total - 1) + 1)
        return jnp.stack([one, total - one])
    sizes = jnp.asarray(length_profile(amount, total, reach, skew), jnp.int32)
    twos = (amount - 1) // 2
    donor, sink = sizes[1:1 + 2 * twos:2], sizes[2:2 + 2 * twos:2]
    margin = jnp.minimum(donor - 1, reach - sink)
    shifted = jax.random.randint(jax.random.fold_in(key, 1), (twos,), 0, 1 << 20) % (margin + 1)
    sizes = sizes.at[1:1 + 2 * twos:2].set(donor - shifted).at[2:2 + 2 * twos:2].set(sink + shifted)
    return sizes[jax.random.permutation(jax.random.fold_in(key, 2), amount)]


def normal_values(own_key, extent, width, limit, cuts=(), held_as=jnp.bfloat16):
    gain = levels(own_key, extent, cuts, -0.22, 0.18) if cuts else 1.0
    array = jax.random.normal(own_key, extent, jnp.float32) * width * gain
    return jnp.minimum(jnp.maximum(array, -limit), limit).astype(held_as)


def setup_inputs(seed: int = 0) -> dict:
    streams_of = jax.random.split(jax.random.key(seed), 7)
    return {
        "layer_inputs": normal_values(streams_of[0], (TASKS, TOK, D), 1.0, 6.0, ((0, 4), (2, 8))),
        "queries": draw_queries(jax.random.fold_in(streams_of[6], 71), 0),
        "key_values": draw_key_values(jax.random.fold_in(streams_of[6], 71), 0),
        "out_grads": normal_values(streams_of[3], (TASKS, TOK, QH * HD), 0.05, 0.29882812, ((0, 4), (2, 8))),
        "lengths": jax.vmap(lambda own: uneven(own, NSEQ, TOK, MAXLEN, 2))(jax.random.split(streams_of[4], TASKS)).reshape((TASKS, NSEQ)).astype(jnp.int32),
        "task_weights": normal_values(streams_of[5], (TASKS, D, KVC), 1.0, 6.0, ((0, 4), (1, 8))),
    }


EPS = 1e-6
NEGATIVE = -1e30


def layout(lengths, count):
    lengths = lengths.astype(jnp.int32)
    ending = jnp.cumsum(lengths).astype(jnp.int32)
    starts = (ending - lengths).astype(jnp.int32)
    places = jnp.arange(count, dtype=jnp.int32)
    owner = jnp.sum((places[:, None] >= ending[None, :]).astype(jnp.int32), axis=1).astype(jnp.int32)
    allowed = (owner[:, None] == owner[None, :]) & (places[:, None] >= places[None, :])
    return owner, starts, allowed


def head_grads(head_query, head_keys, head_values, head_cotangent, allowed):
    factor = HD ** -0.5
    scores = jnp.dot(head_query, head_keys.T, preferred_element_type=jnp.float32) * factor
    scores = jnp.where(allowed, scores, NEGATIVE)
    highest = jnp.max(scores, axis=1, keepdims=True)
    summed = jnp.sum(jnp.exp(scores - highest), axis=1, keepdims=True)
    chances = jnp.where(allowed, jnp.exp(scores - highest - jnp.log(summed)), jnp.zeros_like(scores))
    slopes = jnp.dot(head_cotangent, head_values.T, preferred_element_type=jnp.float32)
    offsets = jnp.sum(chances * slopes, axis=1, keepdims=True)
    score_grads = (chances * (slopes - offsets)).astype(jnp.bfloat16)
    value_grads = jnp.dot(chances.astype(jnp.bfloat16).T, head_cotangent, preferred_element_type=jnp.float32)
    key_grads = jnp.dot(score_grads.T, head_query, preferred_element_type=jnp.float32) * factor
    return jnp.concatenate([key_grads, value_grads], axis=1)


def seq_fisher(inputs, grads_all, owner, starts, number_seqs):
    window = inputs.shape[0] // 2
    last_start = inputs.shape[0] - window

    def one_seq(running, number):
        opening = jnp.clip(starts[number], 0, last_start).astype(jnp.int32)
        rows_in = lax.dynamic_slice_in_dim(inputs, opening, window, 0)
        rows_grad = lax.dynamic_slice_in_dim(grads_all, opening, window, 0)
        inside = lax.dynamic_slice_in_dim(owner, opening, window, 0) == number
        rows_grad = jnp.where(inside[:, None], rows_grad, jnp.zeros_like(rows_grad))
        gradient = jnp.dot(rows_in.T, rows_grad, preferred_element_type=jnp.float32)
        return running + gradient * gradient, None

    start_value = jnp.zeros((inputs.shape[1], grads_all.shape[1]), jnp.float32)
    running, unused = lax.scan(one_seq, start_value, jnp.arange(number_seqs, dtype=jnp.int32))
    return running


def task_part(fields):
    inputs, queries, key_values, cotangents, lengths = fields
    count = inputs.shape[0]
    owner, starts, allowed = layout(lengths, count)
    group_heads = QH // KVH
    run_heads = QH // N_COL

    def kv_block(kv_number):
        block = lax.dynamic_slice_in_dim(key_values, kv_number * 2 * HD, 2 * HD, 1)
        head_keys = block[:, :HD]
        head_values = block[:, HD:]
        summed = jnp.zeros((count, 2 * HD), jnp.float32)
        for run_number in range(group_heads // run_heads):
            partial_sum = jnp.zeros((count, 2 * HD), jnp.float32)
            for member in range(run_heads):
                query_number = kv_number * group_heads + run_number * run_heads + member
                head_query = lax.dynamic_slice_in_dim(queries, query_number * HD, HD, 1)
                head_cotangent = lax.dynamic_slice_in_dim(cotangents, query_number * HD, HD, 1)
                partial_sum = partial_sum + head_grads(head_query, head_keys, head_values, head_cotangent, allowed)
            rounded = lax.optimization_barrier(partial_sum.astype(jnp.bfloat16))
            summed = summed + rounded.astype(jnp.float32)
        return summed.astype(jnp.bfloat16)

    blocks = lax.map(kv_block, jnp.arange(KVH, dtype=jnp.int32))
    grads_all = jnp.transpose(blocks, (1, 0, 2)).reshape(count, KVH * 2 * HD)
    return seq_fisher(inputs, grads_all, owner, starts, lengths.shape[0])


def reference(layer_inputs, queries, key_values, out_grads, lengths, task_weights):
    fisher = lax.map(task_part, (layer_inputs, queries, key_values, out_grads, lengths))
    weighted = jnp.sum(fisher * task_weights.astype(jnp.float32), axis=0)
    divisor = jnp.sum(fisher, axis=0) + EPS
    return fisher, (weighted / divisor).astype(jnp.bfloat16)
```

```python
import functools
import math

import jax
import jax.numpy as jnp
from jax import lax
from jax.experimental import pallas as pl
from jax.experimental.pallas import tpu as pltpu
from jax.sharding import PartitionSpec as P

KVH = 8
HD = 128
PAIR = 2 * HD
EPS = 1e-06
NEGATIVE = -1e30
BLK = 256


NT = (((1,), (1,)), ((), ()))
NN = (((1,), (0,)), ((), ()))


def dot(a, b, dims):
    return lax.dot_general(a, b, dims, preferred_element_type=jnp.float32)


def pick(values, index):
    out = jnp.int32(values[0])
    for at in range(1, len(values)):
        out = jnp.where(index == at, jnp.int32(values[at]), out)
    return out


def xor_permute(value, axis, size, bits):
    return lax.ppermute(value, axis, [(i, i ^ bits) for i in range(size)])


def split_kernel(devices, groups, place, kv, *outs):
    me = place[1]
    for k in range(devices):
        head = (me ^ k) // groups
        outs[k][...] = kv[:, pl.ds(pl.multiple_of(head * PAIR, PAIR), PAIR)]


def split_rows(place, rows, devices):
    out = jax.ShapeDtypeStruct((rows.shape[0], PAIR), rows.dtype)
    return pl.pallas_call(
        functools.partial(split_kernel, devices, devices // KVH),
        in_specs=[pl.BlockSpec(memory_space=pltpu.SMEM), pl.BlockSpec(memory_space=pltpu.VMEM)],
        out_specs=[pl.BlockSpec(memory_space=pltpu.VMEM)] * devices,
        out_shape=[out] * devices,
    )(place, rows)


def visits_of(count, seqs):
    return count // BLK + seqs - 1


def mask_kernel(seqs, visits, lengths, x, out, table):
    starts, ends, at = [], [], jnp.int32(0)
    for s in range(seqs):
        starts.append(at)
        at = at + lengths[s]
        ends.append(at)
    ends.append(at)
    starts.append(at)

    def choose(values, s):
        out = values[-1]
        for i in range(len(values) - 1):
            out = jnp.where(s == i, values[i], out)
        return out

    s, b, cont = jnp.int32(0), jnp.int32(0), jnp.int32(0)
    lane = lax.broadcasted_iota(jnp.int32, (1, BLK), 1)
    for v in range(visits):
        first, end = choose(starts, s), choose(ends, s)
        live = s < seqs
        base = b * BLK
        here = jnp.where(live, b, 0)
        rows = x[pl.ds(pl.multiple_of(here * BLK, BLK), BLK), :]
        keep = (base + lane >= first) & (base + lane < end)
        keep = jnp.where(keep, 1.0, 0.0) * jnp.where(live, 1.0, 0.0)
        turned = rows.astype(jnp.float32).T * keep
        out[:, v * BLK : (v + 1) * BLK] = turned.astype(jnp.bfloat16)
        more = live & (end > base + BLK)
        table[3 * v] = here
        table[3 * v + 1] = cont
        table[3 * v + 2] = jnp.where(more, 0, 1)
        following = choose(starts, s + 1)
        b = jnp.where(more, b + 1, following // BLK)
        s = jnp.where(more, s, jnp.minimum(s + 1, seqs))
        cont = jnp.where(more, 1, 0)


def masked_inputs(lengths, x):
    count, width = x.shape
    seqs = lengths.shape[0]
    visits = visits_of(count, seqs)
    tile = min(width, 256)
    return pl.pallas_call(
        functools.partial(mask_kernel, seqs, visits),
        grid_spec=pltpu.PrefetchScalarGridSpec(
            num_scalar_prefetch=1,
            grid=(width // tile,),
            in_specs=[pl.BlockSpec((count, tile), lambda g, n: (0, g))],
            out_specs=[
                pl.BlockSpec((tile, visits * BLK), lambda g, n: (g, 0)),
                pl.BlockSpec(memory_space=pltpu.SMEM),
            ],
        ),
        out_shape=[
            jax.ShapeDtypeStruct((width, visits * BLK), jnp.bfloat16),
            jax.ShapeDtypeStruct((3 * visits,), jnp.int32),
        ],
        cost_estimate=pl.CostEstimate(
            flops=4 * count * width, transcendentals=0, bytes_accessed=5 * count * width
        ),
    )(lengths, x)


def grads_kernel(devices, heads, lengths, place, q_ref, do_ref, *refs):
    parts, (out_ref, kv_ref, acc_ref, bias_ref) = refs[:devices], refs[devices:]
    step = pl.program_id(0)
    me = place[1]
    rows = parts[0].shape[0]
    seqs = lengths.shape[0]
    scale = HD ** (-0.5) * math.log2(math.e)

    @pl.when(step == 0)
    def _():
        for k in range(devices):
            kv_ref[pl.ds(pl.multiple_of((me ^ k) * rows, rows), rows), :] = parts[k][...]
        acc_ref[...] = jnp.zeros_like(acc_ref)

    token = step * BLK + lax.broadcasted_iota(jnp.int32, (1, BLK), 1)
    begin = jnp.zeros((1, BLK), jnp.int32)
    opening = jnp.int32(0)
    end = jnp.int32(0)
    for s in range(seqs - 1):
        end = end + lengths[s]
        begin = jnp.where(token >= end, end, begin)
        opening = jnp.where(step * BLK >= end, end, opening)
    lowest = opening // BLK
    most = bias_ref.shape[0] // BLK

    for blocks in range(1, most + 1):

        @pl.when(step - lowest + 1 == blocks)
        def _():
            width = blocks * BLK
            base = pl.multiple_of(lowest * BLK, BLK)
            window = pl.ds(base, width)
            key = base + lax.broadcasted_iota(jnp.int32, (width, BLK), 0)
            allowed = (key >= begin) & (key <= token)
            bias_ref[:width, :] = jnp.where(allowed, 0.0, NEGATIVE)

            def one(head):
                cols = pl.ds(pl.multiple_of(head * HD, HD), HD)
                query, cotangent = q_ref[:, cols], do_ref[:, cols]
                scores = dot(kv_ref[window, :HD], query, NT) * scale + bias_ref[:width, :]
                highest = jnp.max(scores, axis=0, keepdims=True)
                powers = jnp.exp2(scores - highest)
                inverse = 1.0 / jnp.sum(powers, axis=0, keepdims=True)
                chances = powers * inverse
                slopes = dot(kv_ref[window, HD:], cotangent, NT)
                offsets = jnp.sum(chances * slopes, axis=0, keepdims=True)
                score_grads = (chances * (slopes - offsets)).astype(jnp.bfloat16)
                value_grads = dot(chances.astype(jnp.bfloat16), cotangent, NN)
                key_grads = dot(score_grads, query, NN)
                return key_grads, value_grads

            unroll = 2 if heads % 2 == 0 else 1

            def body(at, carry):
                keys, values = one(at * unroll)
                for more in range(1, unroll):
                    extra = one(at * unroll + more)
                    keys, values = keys + extra[0], values + extra[1]
                acc_ref[window, :HD] += keys
                acc_ref[window, HD:] += values
                return carry

            lax.fori_loop(0, heads // unroll, body, 0)

    @pl.when(step == pl.num_programs(0) - 1)
    def _():
        out_ref[:, :HD] = (acc_ref[:, :HD] * HD ** (-0.5)).astype(jnp.bfloat16)
        out_ref[:, HD:] = acc_ref[:, HD:].astype(jnp.bfloat16)


def run_grads(lengths, place, queries, cotangents, parts):
    count, width = queries.shape
    devices, heads = len(parts), width // HD
    most = count // 2 // BLK + 1
    whole = pl.BlockSpec(parts[0].shape, lambda g, n, p: (0, 0))
    return pl.pallas_call(
        functools.partial(grads_kernel, devices, heads),
        grid_spec=pltpu.PrefetchScalarGridSpec(
            num_scalar_prefetch=2,
            grid=(count // BLK,),
            in_specs=[
                pl.BlockSpec((BLK, width), lambda g, n, p: (g, 0)),
                pl.BlockSpec((BLK, width), lambda g, n, p: (g, 0)),
            ]
            + [whole] * devices,
            out_specs=pl.BlockSpec((count, PAIR), lambda g, n, p: (0, 0)),
            scratch_shapes=[
                pltpu.VMEM((count, PAIR), jnp.bfloat16),
                pltpu.VMEM((count, PAIR), jnp.float32),
                pltpu.VMEM((most * BLK, BLK), jnp.float32),
            ],
        ),
        out_shape=jax.ShapeDtypeStruct((count, PAIR), jnp.bfloat16),
        compiler_params=pltpu.CompilerParams(vmem_limit_bytes=48 << 20),
        cost_estimate=pl.CostEstimate(
            flops=8 * count * count * width // 2,
            transcendentals=count * count * heads // 2,
            bytes_accessed=4 * count * width,
        ),
    )(lengths, place, queries, cotangents, *parts)


def order_of(step, size):
    bits = size.bit_length() - 1
    out = jnp.int32(0)
    for b in range(bits):
        out = out | ((((size - 1 - step) >> (bits - 1 - b)) & 1) << b)
    return out


def fisher_kernel(blocks, visits, half, table, place, x_ref, *refs):
    grads, w_ref = refs[:blocks], refs[blocks]
    fisher_ref, send_ref, keep_ref, tile_ref = refs[-4:]
    step, which = pl.program_id(0), pl.program_id(1)
    for k in range(blocks):

        @pl.when(which == k)
        def _():
            total = None
            running = None
            for v in range(visits):
                base = pl.multiple_of(table[3 * v] * BLK, BLK)
                got = dot(x_ref[:, v * BLK : (v + 1) * BLK], grads[k][pl.ds(base, BLK), :], NN)
                if v:
                    got = got + running * table[3 * v + 1].astype(jnp.float32)
                running = got
                square = got * (got * table[3 * v + 2].astype(jnp.float32))
                total = square if total is None else total + square
            tile_ref[...] = total

    total = tile_ref[...]
    fisher_ref[...] = total
    weighted = (total * w_ref[...].astype(jnp.float32)).astype(jnp.bfloat16)
    rounded = total.astype(jnp.bfloat16)

    @pl.when(step < half)
    def _():
        send_ref[0, 0] = weighted
        send_ref[0, 1] = rounded

    @pl.when(step >= half)
    def _():
        keep_ref[0, 0] = weighted
        keep_ref[0, 1] = rounded


def fisher_of(tasks, table, place, x, grads, heads_of, weights, before):
    rows = x.shape[0]
    count = grads[0].shape[0]
    blocks, half, tile = len(grads), tasks // 2, rows // tasks
    visits = x.shape[1] // BLK

    def row(g, p):
        return p[0] ^ order_of(g, tasks)

    def send_map(g, h, t, p):
        return (jnp.minimum(g, half - 1), 0, 0, jnp.where(g < half, h, blocks - 1))

    def keep_map(g, h, t, p):
        return (jnp.maximum(g - half, 0), 0, 0, jnp.where(g < half, 0, h))

    place_map = lambda g, h, t, p: (row(g, p), heads_of(h, p))
    in_specs = [pl.BlockSpec((tile, visits * BLK), lambda g, h, t, p: (row(g, p), 0))]
    in_specs += [pl.BlockSpec((count, PAIR), lambda g, h, t, p: (0, 0))] * blocks
    in_specs += [pl.BlockSpec((tile, PAIR), place_map)]
    args = [table, place, x, *grads, weights]
    aliases = {}
    if before is not None:
        in_specs.append(pl.BlockSpec(memory_space=pl.ANY))
        aliases = {len(args): 0}
        args.append(before)
    sums = jax.ShapeDtypeStruct((half, 2, tile, blocks * PAIR), jnp.bfloat16)
    return pl.pallas_call(
        functools.partial(fisher_kernel, blocks, visits, half),
        grid_spec=pltpu.PrefetchScalarGridSpec(
            num_scalar_prefetch=2,
            grid=(tasks, blocks),
            in_specs=in_specs,
            out_specs=[
                pl.BlockSpec((tile, PAIR), place_map),
                pl.BlockSpec((1, 2, tile, PAIR), send_map),
                pl.BlockSpec((1, 2, tile, PAIR), keep_map),
            ],
            scratch_shapes=[pltpu.VMEM((tile, PAIR), jnp.float32)],
        ),
        out_shape=[jax.ShapeDtypeStruct(weights.shape, jnp.float32), sums, sums],
        input_output_aliases=aliases,
        cost_estimate=pl.CostEstimate(
            flops=2 * rows * visits * BLK * blocks * PAIR,
            transcendentals=0,
            bytes_accessed=12 * rows * blocks * PAIR,
        ),
    )(*args)


def place_kernel(tasks, place, *refs):
    pieces, out_ref = refs[:tasks], refs[-1]
    step = pl.program_id(0)
    for i in range(tasks):

        @pl.when(step == i)
        def _():
            out_ref[...] = pieces[i][...]


def place_rows(tasks, place, pieces, heads_of, shape, before):
    tile, width = pieces[0].shape
    blocks = width // PAIR
    in_specs = [pl.BlockSpec((tile, PAIR), lambda g, h, p: (0, h))] * tasks
    args = [place, *pieces]
    aliases = {}
    if before is not None:
        in_specs = in_specs + [pl.BlockSpec(memory_space=pl.ANY)]
        aliases = {len(args): 0}
        args.append(before)
    return pl.pallas_call(
        functools.partial(place_kernel, tasks),
        grid_spec=pltpu.PrefetchScalarGridSpec(
            num_scalar_prefetch=1,
            grid=(tasks, blocks),
            in_specs=in_specs,
            out_specs=pl.BlockSpec((tile, PAIR), lambda g, h, p: (p[0] ^ g, heads_of(h, p))),
        ),
        out_shape=jax.ShapeDtypeStruct(shape, jnp.bfloat16),
        input_output_aliases=aliases,
        cost_estimate=pl.CostEstimate(
            flops=tasks * tile * width, transcendentals=0, bytes_accessed=4 * tasks * tile * width
        ),
    )(*args)


def merge_rows(tasks, send, keep):
    bit = 1
    while True:
        got = xor_permute(send, "task", tasks, bit)
        total = keep.astype(jnp.float32) + got.astype(jnp.float32)
        bit *= 2
        if bit == tasks:
            break
        half = total.shape[0] // 2
        send, keep = total[:half].astype(jnp.bfloat16), total[half:]
    return (total[0, 0] / (total[0, 1] + EPS)).astype(jnp.bfloat16)


def spread_rows(tasks, piece):
    pieces = {0: piece}
    bit = tasks // 2
    while bit:
        pieces.update({at | bit: xor_permute(pieces[at], "task", tasks, bit) for at in list(pieces)})
        bit //= 2
    return [pieces[at] for at in range(tasks)]


def body(layer_inputs, queries, key_values, out_grads, lengths, task_weights):
    devices, tasks = lax.axis_size("col"), lax.axis_size("task")
    groups = devices // KVH
    place = jnp.stack([lax.axis_index("task"), lax.axis_index("col")]).astype(jnp.int32)
    sizes = lengths[0]
    weights = task_weights[0]

    parts = split_rows(place, key_values[0], devices)
    parts = [parts[0]] + [xor_permute(parts[k], "col", devices, k) for k in range(1, devices)]
    turned, table = masked_inputs(sizes, layer_inputs[0])
    own = run_grads(sizes, place, queries[0], out_grads[0], parts)

    if groups == 1:
        blocks = {0: own, 1: xor_permute(own, "col", devices, 1)}
        for k in range(2, devices, 2):
            blocks[k] = xor_permute(own, "col", devices, k)
            blocks[k + 1] = xor_permute(blocks[k], "col", devices, 1)
        blocks = [blocks[k] for k in range(devices)]
        head_at = lambda k, p: p[1] ^ k
    else:
        runs = lax.all_gather(own, "col", axis=0, tiled=False)
        runs = runs.reshape((KVH, groups) + own.shape).astype(jnp.float32)
        heads = jnp.sum(runs, axis=1).astype(jnp.bfloat16)
        blocks = [heads[k] for k in range(KVH)]
        head_at = lambda k, p: k

    chunks = [[0], [1, 2], [3, 4], [5, 6], [7]]
    fisher, merged = None, None
    for chunk in chunks:
        heads_of = lambda h, p, chunk=chunk: head_at(pick(chunk, h), p)
        fisher, send, keep = fisher_of(
            tasks, table, place, turned, [blocks[k] for k in chunk], heads_of, weights, fisher
        )
        piece = merge_rows(tasks, send, keep)
        pieces = spread_rows(tasks, piece)
        merged = place_rows(tasks, place, pieces, heads_of, weights.shape, merged)
    return fisher[None], merged


def solution(mesh):
    in_specs = (
        P("task", None, "col"),
        P("task", None, "col"),
        P("task", "col", None),
        P("task", None, "col"),
        P("task", None),
        P("task", "col", None),
    )
    out_specs = (P("task", "col", None), P("col", None))
    return jax.shard_map(body, mesh=mesh, in_specs=in_specs, out_specs=out_specs, check_vma=False)
```
